32 devices in a mesh: vp: 8 (over z, y), rep: 4 (over x, core).
Axes of the slice: x: 2, y: 2, z: 4, core: 2. Of those that a mesh axis runs over, the one named last changes fastest.
Arguments:
- features: bfloat16 [65536, 256], P(('vp', 'rep')), may hold values from -48 to 48
- tile_values: bfloat16 [8192, 128, 128], P(('vp', 'rep')), may hold values from 0 to 0.0014648438
- tile_cols: int32 [8192], P(('vp', 'rep')), may hold values from 0 to 31, as said below
- halo_rows: int32 [32, 4, 4], P(('vp', 'rep')), may hold values from 0 to 15
Outputs:
- scores: bfloat16 [65536, 256], P(('vp', 'rep'))
The draws below stay inside these ranges and needn't reach their ends.
Inputs may be any that keep to these rules, and one draw needn't show every extreme that they name: `tile_cols`: values below 16 name one of the shard's own row blocks; value 16 + o * 4 + j names the j-th block sent by peer o. Every value occurs on every shard.
All inputs are finite; a program needn't handle non-finite values.
Results may differ from the reference program's by a relative error of at most 0.002.
Values may be sent and summed in bfloat16 or wider, within the bound.
A program may use at most 128 MiB of HBM per device.

```python
import math
import jax
import jax.numpy as jnp
from jax import lax

CLASSES = 256
TILE = 128
BLOCKS_DEV = 16
TILES_ROW = 16
HALO_SLOTS = 4
ITERS = 3
SHARDS = 32
VERTICES = 65536
TILES = 8192


def draw_features(key, part):
    scale_key, noise_key, common_key = jax.random.split(key, 3)
    block_count = SHARDS * BLOCKS_DEV
    scales = jnp.exp(jax.random.uniform(scale_key, (block_count, 1, 1), minval=0.0, maxval=math.log(8.0)))
    noise = jnp.clip(jax.random.normal(noise_key, (block_count, TILE, CLASSES)), -6.0, 6.0)
    values = scales * noise
    values = jnp.clip(values, -48.0, 48.0).reshape(block_count * TILE, CLASSES)
    return values.astype(jnp.bfloat16)


def draw_tile_cols(key, part):
    slot_count = BLOCKS_DEV + 4 * HALO_SLOTS
    per_device = BLOCKS_DEV * TILES_ROW
    device_keys = jax.random.split(key, SHARDS)

    def one_device(device_key):
        first_key, second_key = jax.random.split(device_key)
        base_slots = jax.random.randint(first_key, (per_device,), 0, slot_count, dtype=jnp.int32)
        placing = jax.random.permutation(second_key, per_device)
        return base_slots.at[placing[:slot_count]].set(jnp.arange(slot_count, dtype=jnp.int32))
    return jax.vmap(one_device)(device_keys).reshape(-1)


def with_ends(entries, key, least, top_value):
    index_at = [jax.random.randint(jax.random.fold_in(key, axis), (), 0, length) for axis, length in enumerate(entries.shape)]
    main_axis = entries.shape.index(max(entries.shape))
    next_to = index_at[:main_axis] + [(index_at[main_axis] + 1) % entries.shape[main_axis]] + index_at[main_axis + 1:]
    return entries.at[tuple(index_at)].set(least).at[tuple(next_to)].set(top_value)


def levels(key, extent, cuts, least, largest):
    gain, own = 1.0, jax.random.fold_in(key, 6)
    for dim, parts in cuts:
        heights = jnp.exp(jax.random.uniform(jax.random.fold_in(own, dim), (parts,), jnp.float32, least / len(cuts), largest / len(cuts)))
        gain = gain * jnp.repeat(heights, extent[dim] // parts).reshape([-1 if axis == dim else 1 for axis in range(len(extent))])
    return gain


def setup_inputs(seed: int = 0) -> dict:
    seeds = jax.random.split(jax.random.key(seed), 5)
    return {
        "features": draw_features(jax.random.fold_in(seeds[4], 71), 0),
        "tile_values": jnp.clip(0.0014648438 * jax.random.uniform(seeds[1], (TILES, TILE, TILE), jnp.float32) ** levels(seeds[1], (TILES, TILE, TILE), ((0, 32),), -0.2, 0.2), 0.0, 0.0014648438).astype(jnp.bfloat16),
        "tile_cols": draw_tile_cols(jax.random.fold_in(seeds[4], 71), 0),
        "halo_rows": with_ends(jax.random.randint(seeds[3], (SHARDS, 4, HALO_SLOTS), 0, BLOCKS_DEV), jax.random.fold_in(seeds[3], 1), 0, BLOCKS_DEV - 1).astype(jnp.int32),
    }


def reference(features, tile_values, tile_cols, halo_rows):
    nblocks = BLOCKS_DEV
    tiles_dev = BLOCKS_DEV * TILES_ROW
    device_ids = jnp.arange(SHARDS, dtype=jnp.int32)
    slots = tile_cols.reshape(SHARDS, tiles_dev).astype(jnp.int32)
    is_local = slots < nblocks
    halo_slot = jnp.maximum(slots - nblocks, 0)
    offset_slot = (halo_slot // HALO_SLOTS).astype(jnp.int32)
    slot_entry = (halo_slot % HALO_SLOTS).astype(jnp.int32)
    shift_by = jnp.array([1, -1, 4, -4], dtype=jnp.int32)[offset_slot]
    sender = ((device_ids[:, None] - shift_by) % SHARDS).astype(jnp.int32)
    sent_block = halo_rows[sender, offset_slot, slot_entry].astype(jnp.int32)
    source_block = jnp.where(is_local, device_ids[:, None] * nblocks + slots, sender * nblocks + sent_block).astype(jnp.int32)
    source_block = source_block.reshape(SHARDS, nblocks, TILES_ROW)
    tiles = tile_values.reshape(SHARDS, nblocks, TILES_ROW, TILE, TILE)
    teleport_part = 0.1 * features.astype(jnp.float32)
    current = features
    for iteration in range(ITERS):
        blocks = current.reshape(SHARDS * nblocks, TILE, CLASSES)

        def propagate_device(pair):
            tiles_here, sources_here = pair
            gathered = blocks[sources_here]
            return jnp.einsum('rtij,rtjc->ric', tiles_here.astype(jnp.float32), gathered.astype(jnp.float32), precision=lax.Precision.HIGHEST)
        propagated = lax.map(propagate_device, (tiles, source_block)).reshape(VERTICES, CLASSES)
        blended = 0.9 * propagated + teleport_part
        total_mass = lax.optimization_barrier(jnp.sum(blended * blended, axis=0))
        current = (blended / jnp.sqrt(0.05 + total_mass / VERTICES)).astype(jnp.bfloat16)
    return current
```

```python
import functools

import jax
import jax.numpy as jnp
from jax import lax
from jax.experimental import pallas as pl
from jax.experimental.pallas import tpu as pltpu
from jax.sharding import PartitionSpec as P

ITERS = 3
LANES = 128
MESH = pl.DeviceIdType.MESH
LOADS = 8
UNROLL = 64


def kernel(vp_count, rep_count, vertices, slots, halves, *refs):
    cols_ref, rows_ref, feat_hbm, tiles_hbm, out_hbm = refs[:5]
    it_refs = iter(refs[5:])
    take = lambda count: [next(it_refs) for _ in range(count)]
    tiles = take(1)[0]
    tables = [take(halves) for _ in range(ITERS)]
    feats = take(halves)
    owns = take(halves)
    sends = [take(halves) for _ in range(ITERS)]
    finals = take(halves)
    stages = take(halves)
    mine = [take(halves) for _ in range(ITERS)]
    got = [take(halves) for _ in range(ITERS)]
    order, place = take(2)
    (tile_sem, feat_sem, table_sem, out_sem, send_sem, recv_sem, mass_send, mass_recv) = take(8)

    nblocks, tile_size = feats[0].shape[0], feats[0].shape[1]
    ntiles = tiles.shape[0]
    per_row = ntiles // nblocks
    my_vp, my_rep = lax.axis_index("vp"), lax.axis_index("rep")
    me = my_vp * rep_count + my_rep
    shards = vp_count * rep_count

    own_loads, table_loads = [], []
    for h in range(halves):
        part = feat_hbm.at[:, :, pl.ds(h * LANES, LANES)]
        own_loads.append(pltpu.make_async_copy(part, feats[h], feat_sem.at[h]))
        table_loads.append(
            pltpu.make_async_copy(part, tables[0][h].at[pl.ds(0, nblocks)], table_sem.at[h])
        )
    for h in range(halves):
        own_loads[h].start()
    for h in range(halves):
        table_loads[h].start()
    chunk = ntiles // LOADS
    tile_loads = []
    for k in range(LOADS):
        piece = pl.ds(k * chunk, chunk)
        tile_loads.append(pltpu.make_async_copy(tiles_hbm.at[piece], tiles.at[piece], tile_sem.at[k]))
        tile_loads[-1].start()

    def device_at(distance):
        flat = lax.rem(me + distance + shards, shards)
        return flat // rep_count, lax.rem(flat, rep_count)

    def peer_at(o):
        size = 1 + 3 * (o // 2)
        return device_at(size * (1 - 2 * lax.rem(o, 2)))

    barrier = pltpu.get_barrier_semaphore()

    def greet(k, carry):
        pl.semaphore_signal(barrier, inc=1, device_id=device_at(k), device_id_type=MESH)
        return carry

    lax.fori_loop(1, shards, greet, 0)

    def sent(o, j):
        return rows_ref[0, o, j]

    turns = []
    for b in range(nblocks):
        turn = jnp.int32(4)
        for g in reversed(range(4)):
            hit = sent((g + 2) % 4, 0) == b
            for j in range(1, slots):
                hit = hit | (sent((g + 2) % 4, j) == b)
            turn = jnp.where(hit, g, turn)
        turns.append(turn * nblocks + b)
    places = []
    for b in range(nblocks):
        at = jnp.int32(0)
        for c in range(nblocks):
            if c != b:
                at = at + jnp.where(turns[c] < turns[b], 1, 0)
        places.append(at)
        place[b] = at
    for b in range(4 * slots):
        place[nblocks + b] = jnp.int32(nblocks + b)
    for k in range(nblocks):
        row = jnp.int32(0)
        for b in range(nblocks):
            row = row + jnp.where(places[b] == k, b, 0)
        order[k] = row

    pl.semaphore_wait(barrier, shards - 1)

    def halo_copy(it, h, o):
        at = (it * halves + h) * 4 + o
        return pltpu.make_async_remote_copy(
            src_ref=sends[it][h].at[pl.ds(o * slots, slots)],
            dst_ref=tables[it][h].at[pl.ds(nblocks + o * slots, slots)],
            send_sem=send_sem.at[at],
            recv_sem=recv_sem.at[at],
            device_id=peer_at(o),
            device_id_type=MESH,
        )

    def send_halo(it, h, o, source):
        for j in range(slots):
            row = rows_ref[0, o, j]
            sends[it][h][o * slots + j] = source[place[row] if it else row]
        halo_copy(it, h, o).start()

    def mass_copy(it, h, k):
        at = it * halves + h
        return pltpu.make_async_remote_copy(
            src_ref=mine[it][h],
            dst_ref=got[it][h].at[k - 1],
            send_sem=mass_send.at[at],
            recv_sem=mass_recv.at[at],
            device_id=device_at(k),
            device_id_type=MESH,
        )

    def mass_all(it, h):
        at = it * halves + h
        return pltpu.make_async_remote_copy(
            src_ref=got[it][h],
            dst_ref=got[it][h],
            send_sem=mass_send.at[at],
            recv_sem=mass_recv.at[at],
            device_id=device_at(1),
            device_id_type=MESH,
        )

    def mass_first(it, h, mass):
        mine[it][h][...] = mass

        def one(k, carry):
            mass_copy(it, h, k).start()
            return carry

        lax.fori_loop(1, shards, one, 0, unroll=shards <= UNROLL)

    def mass_total(it, h):
        mass_all(it, h).wait_recv()
        total = mine[it][h][...] + jnp.sum(got[it][h][...], axis=0)
        return 1.0 / jnp.sqrt(0.05 + total / vertices)

    def propagate(it, h, gain):
        table = tables[it][h]
        last = it + 1 == ITERS

        def row(k, mass):
            r = k if last else order[k]
            first = r * per_row
            slot = lambda t: cols_ref[first + t]
            source = slot if it == 0 else lambda t: place[slot(t)]
            left = jnp.concatenate([tiles[first + t] for t in range(per_row)], axis=1)
            right = jnp.concatenate([table[source(t)] for t in range(per_row)], axis=0)
            total = jnp.dot(left, right, preferred_element_type=jnp.float32)
            blended = gain * total + 0.1 * feats[h][r].astype(jnp.float32)
            if last:
                finals[h][k] = blended
            else:
                rounded = blended.astype(jnp.bfloat16)
                owns[h][k] = rounded
                tables[it + 1][h][k] = rounded
            squares = (blended * blended).reshape(tile_size // 8, 8, LANES)
            return mass + jnp.sum(squares, axis=0)

        def group(g, mass):
            for k in range(nblocks // 4):
                mass = row(g * (nblocks // 4) + k, mass)
            if not last:
                send_halo(it + 1, h, lax.rem(g + 2, 4), owns[h])
            return mass

        mass = lax.fori_loop(0, 4, group, jnp.zeros((8, LANES), jnp.float32))
        return jnp.sum(mass, axis=0, keepdims=True)

    for h in range(halves):
        own_loads[h].wait()
        for o in (2, 3, 0, 1):
            send_halo(0, h, o, feats[h])
    for h in range(halves):
        table_loads[h].wait()
    for load in tile_loads:
        load.wait()

    def finish(h):
        scale = mass_total(ITERS - 1, h)
        for b in range(nblocks):
            stages[h][b] = (finals[h][b] * scale).astype(jnp.bfloat16)
        pltpu.make_async_copy(
            stages[h], out_hbm.at[:, :, pl.ds(h * LANES, LANES)], out_sem.at[h]
        ).start()

    for it in range(ITERS):
        for h in range(halves):
            for o in range(4):
                halo_copy(it, h, o).wait_recv()
            gain = 0.9 if it == 0 else 0.9 * mass_total(it - 1, h)
            mass = propagate(it, h, gain)
            mass_first(it, h, mass)
    for h in range(halves):
        finish(h)
    for it in range(ITERS):
        for h in range(halves):
            for o in range(4):
                halo_copy(it, h, o).wait_send()
            mass_all(it, h).wait_send()
    for h in range(halves):
        pltpu.make_async_copy(
            stages[h], out_hbm.at[:, :, pl.ds(h * LANES, LANES)], out_sem.at[h]
        ).wait()


def local(vp_count, rep_count, features, tile_values, tile_cols, halo_rows):
    tile_size = tile_values.shape[1]
    rows, classes = features.shape
    nblocks = rows // tile_size
    slots = halo_rows.shape[2]
    halves = classes // LANES
    shards = vp_count * rep_count
    block = (tile_size, LANES)
    bf16, f32 = jnp.bfloat16, jnp.float32
    each = ITERS * halves
    scratch = [pltpu.VMEM(tile_values.shape, bf16)]
    scratch += [pltpu.VMEM((nblocks + 4 * slots,) + block, bf16)] * each
    scratch += [pltpu.VMEM((nblocks,) + block, bf16)] * (2 * halves)
    scratch += [pltpu.VMEM((4 * slots,) + block, bf16)] * each
    scratch += [pltpu.VMEM((nblocks,) + block, f32)] * halves
    scratch += [pltpu.VMEM((nblocks,) + block, bf16)] * halves
    scratch += [pltpu.VMEM((1, LANES), f32)] * each
    scratch += [pltpu.VMEM((shards - 1, 1, LANES), f32)] * each
    scratch += [pltpu.SMEM((nblocks,), jnp.int32), pltpu.SMEM((nblocks + 4 * slots,), jnp.int32)]
    dma = lambda *shape: pltpu.SemaphoreType.DMA(shape)
    scratch += [dma(LOADS), dma(halves), dma(halves), dma(halves), dma(each * 4), dma(each * 4)]
    scratch += [dma(each)] * 2
    out = pl.pallas_call(
        functools.partial(kernel, vp_count, rep_count, rows * shards, slots, halves),
        out_shape=jax.ShapeDtypeStruct((nblocks, tile_size, classes), bf16),
        in_specs=[pl.BlockSpec(memory_space=pltpu.SMEM)] * 2
        + [pl.BlockSpec(memory_space=pl.ANY)] * 2,
        out_specs=pl.BlockSpec(memory_space=pl.ANY),
        scratch_shapes=scratch,
        compiler_params=pltpu.CompilerParams(
            collective_id=0, has_side_effects=True, vmem_limit_bytes=60 * 1024 * 1024
        ),
    )(tile_cols, halo_rows, features.reshape(nblocks, tile_size, classes), tile_values)
    return out.reshape(rows, classes)


def solution(mesh):
    return jax.shard_map(
        functools.partial(local, mesh.shape["vp"], mesh.shape["rep"]),
        mesh=mesh,
        in_specs=(
            P(("vp", "rep"), None),
            P(("vp", "rep"), None, None),
            P(("vp", "rep")),
            P(("vp", "rep"), None, None),
        ),
        out_specs=P(("vp", "rep"), None),
        check_vma=False,
    )
```

```python
import functools

import jax
import jax.numpy as jnp
from jax import lax
from jax.experimental import pallas as pl
from jax.experimental.pallas import tpu as pltpu
from jax.sharding import PartitionSpec as P

ITERS = 3
LANES = 128
MESH = pl.DeviceIdType.MESH
LOADS = 8
UNROLL = 64
VMEM_LIMIT = 40 * 1024 * 1024


def kernel(vp_count, rep_count, vertices, slots, halves, *refs):
    cols_hbm, rows_hbm, feat_hbm, tiles_hbm, finals_ref, scale_ref = refs[:6]
    it_refs = iter(refs[6:])
    take = lambda count: [next(it_refs) for _ in range(count)]
    tiles = take(1)[0]
    tables = [take(halves) for _ in range(ITERS)]
    feats = take(halves)
    owns = take(halves)
    sends = [take(halves) for _ in range(ITERS)]
    mine = [take(halves) for _ in range(ITERS)]
    got = [take(halves) for _ in range(ITERS)]
    order, place, cols_ref, rows_ref = take(4)
    (index_sem, tile_sem, feat_sem, table_sem, send_sem, recv_sem, mass_send, mass_recv) = take(8)

    nblocks, tile_size = feats[0].shape[0], feats[0].shape[1]
    ntiles = tiles.shape[0]
    per_row = ntiles // nblocks
    my_vp, my_rep = lax.axis_index("vp"), lax.axis_index("rep")
    me = my_vp * rep_count + my_rep
    shards = vp_count * rep_count

    cols_load = pltpu.make_async_copy(cols_hbm, cols_ref, index_sem.at[0])
    rows_load = pltpu.make_async_copy(rows_hbm, rows_ref, index_sem.at[1])
    rows_load.start()
    cols_load.start()
    own_loads, table_loads = [], []
    for h in range(halves):
        part = feat_hbm.at[:, :, pl.ds(h * LANES, LANES)]
        own_loads.append(pltpu.make_async_copy(part, feats[h], feat_sem.at[h]))
        table_loads.append(
            pltpu.make_async_copy(part, tables[0][h].at[pl.ds(0, nblocks)], table_sem.at[h])
        )
    for h in range(halves):
        own_loads[h].start()
    for h in range(halves):
        table_loads[h].start()
    chunk = ntiles // LOADS
    tile_loads = []
    for k in range(LOADS):
        piece = pl.ds(k * chunk, chunk)
        tile_loads.append(pltpu.make_async_copy(tiles_hbm.at[piece], tiles.at[piece], tile_sem.at[k]))
        tile_loads[-1].start()

    def device_at(distance):
        flat = lax.rem(me + distance + shards, shards)
        return flat // rep_count, lax.rem(flat, rep_count)

    def peer_at(o):
        size = 1 + 3 * (o // 2)
        return device_at(size * (1 - 2 * lax.rem(o, 2)))

    barrier = pltpu.get_barrier_semaphore()

    def greet(k, carry):
        pl.semaphore_signal(barrier, inc=1, device_id=device_at(k), device_id_type=MESH)
        return carry

    lax.fori_loop(1, shards, greet, 0)

    rows_load.wait()
    cols_load.wait()

    def sent(o, j):
        return rows_ref[0, o, j]

    turns = []
    for b in range(nblocks):
        turn = jnp.int32(4)
        for g in reversed(range(4)):
            hit = sent((g + 2) % 4, 0) == b
            for j in range(1, slots):
                hit = hit | (sent((g + 2) % 4, j) == b)
            turn = jnp.where(hit, g, turn)
        turns.append(turn * nblocks + b)
    places = []
    for b in range(nblocks):
        at = jnp.int32(0)
        for c in range(nblocks):
            if c != b:
                at = at + jnp.where(turns[c] < turns[b], 1, 0)
        places.append(at)
        place[b] = at
    for b in range(4 * slots):
        place[nblocks + b] = jnp.int32(nblocks + b)
    for k in range(nblocks):
        row = jnp.int32(0)
        for b in range(nblocks):
            row = row + jnp.where(places[b] == k, b, 0)
        order[k] = row

    pl.semaphore_wait(barrier, shards - 1)

    def halo_copy(it, h, o):
        at = (it * halves + h) * 4 + o
        return pltpu.make_async_remote_copy(
            src_ref=sends[it][h].at[pl.ds(o * slots, slots)],
            dst_ref=tables[it][h].at[pl.ds(nblocks + o * slots, slots)],
            send_sem=send_sem.at[at],
            recv_sem=recv_sem.at[at],
            device_id=peer_at(o),
            device_id_type=MESH,
        )

    def send_halo(it, h, o, source):
        for j in range(slots):
            row = rows_ref[0, o, j]
            sends[it][h][o * slots + j] = source[place[row] if it else row]
        halo_copy(it, h, o).start()

    def mass_copy(it, h, k):
        at = it * halves + h
        return pltpu.make_async_remote_copy(
            src_ref=mine[it][h],
            dst_ref=got[it][h].at[k - 1],
            send_sem=mass_send.at[at],
            recv_sem=mass_recv.at[at],
            device_id=device_at(k),
            device_id_type=MESH,
        )

    def mass_all(it, h):
        at = it * halves + h
        return pltpu.make_async_remote_copy(
            src_ref=got[it][h],
            dst_ref=got[it][h],
            send_sem=mass_send.at[at],
            recv_sem=mass_recv.at[at],
            device_id=device_at(1),
            device_id_type=MESH,
        )

    def mass_first(it, h, mass):
        mine[it][h][...] = mass

        def one(k, carry):
            mass_copy(it, h, k).start()
            return carry

        lax.fori_loop(1, shards, one, 0, unroll=shards <= UNROLL)

    def mass_total(it, h):
        mass_all(it, h).wait_recv()
        total = mine[it][h][...] + jnp.sum(got[it][h][...], axis=0)
        return 1.0 / jnp.sqrt(0.05 + total / vertices)

    def propagate(it, h, gain):
        table = tables[it][h]
        last = it + 1 == ITERS

        def row(k, mass):
            r = k if last else order[k]
            first = r * per_row
            slot = lambda t: cols_ref[first + t]
            source = slot if it == 0 else lambda t: place[slot(t)]
            left = jnp.concatenate([tiles[first + t] for t in range(per_row)], axis=1)
            right = jnp.concatenate([table[source(t)] for t in range(per_row)], axis=0)
            total = jnp.dot(left, right, preferred_element_type=jnp.float32)
            blended = gain * total + 0.1 * feats[h][r].astype(jnp.float32)
            if last:
                finals_ref[k, :, h * LANES:(h + 1) * LANES] = blended
            else:
                rounded = blended.astype(jnp.bfloat16)
                owns[h][k] = rounded
                tables[it + 1][h][k] = rounded
            squares = (blended * blended).reshape(tile_size // 8, 8, LANES)
            return mass + jnp.sum(squares, axis=0)

        def group(g, mass):
            for k in range(nblocks // 4):
                mass = row(g * (nblocks // 4) + k, mass)
            if not last:
                send_halo(it + 1, h, lax.rem(g + 2, 4), owns[h])
            return mass

        mass = lax.fori_loop(0, 4, group, jnp.zeros((8, LANES), jnp.float32))
        return jnp.sum(mass, axis=0, keepdims=True)

    for h in range(halves):
        own_loads[h].wait()
        for o in (2, 3, 0, 1):
            send_halo(0, h, o, feats[h])
    for h in range(halves):
        table_loads[h].wait()
    for load in tile_loads:
        load.wait()

    def finish(h):
        scale_ref[:, h * LANES:(h + 1) * LANES] = mass_total(ITERS - 1, h)

    for it in range(ITERS):
        for h in range(halves):
            for o in range(4):
                halo_copy(it, h, o).wait_recv()
            gain = 0.9 if it == 0 else 0.9 * mass_total(it - 1, h)
            mass = propagate(it, h, gain)
            mass_first(it, h, mass)
    for h in range(halves):
        finish(h)
    for it in range(ITERS):
        for h in range(halves):
            for o in range(4):
                halo_copy(it, h, o).wait_send()
            mass_all(it, h).wait_send()


def local(vp_count, rep_count, features, tile_values, tile_cols, halo_rows):
    tile_size = tile_values.shape[1]
    rows, classes = features.shape
    nblocks = rows // tile_size
    slots = halo_rows.shape[2]
    halves = classes // LANES
    shards = vp_count * rep_count
    block = (tile_size, LANES)
    bf16, f32 = jnp.bfloat16, jnp.float32
    each = ITERS * halves
    scratch = [pltpu.VMEM(tile_values.shape, bf16)]
    scratch += [pltpu.VMEM((nblocks + 4 * slots,) + block, bf16)] * each
    scratch += [pltpu.VMEM((nblocks,) + block, bf16)] * (2 * halves)
    scratch += [pltpu.VMEM((4 * slots,) + block, bf16)] * each
    scratch += [pltpu.VMEM((1, LANES), f32)] * each
    scratch += [pltpu.VMEM((shards - 1, 1, LANES), f32)] * each
    scratch += [pltpu.SMEM((nblocks,), jnp.int32), pltpu.SMEM((nblocks + 4 * slots,), jnp.int32)]
    scratch += [pltpu.SMEM(tile_cols.shape, jnp.int32), pltpu.SMEM(halo_rows.shape, jnp.int32)]
    dma = lambda *shape: pltpu.SemaphoreType.DMA(shape)
    scratch += [dma(2), dma(LOADS), dma(halves), dma(halves), dma(each * 4), dma(each * 4)]
    scratch += [dma(each)] * 2
    operands = (tile_cols, halo_rows, features.reshape(nblocks, tile_size, classes), tile_values)
    finals, scale = pl.pallas_call(
        functools.partial(kernel, vp_count, rep_count, rows * shards, slots, halves),
        out_shape=(
            pltpu.VMEM((nblocks, tile_size, classes), f32),
            pltpu.VMEM((1, classes), f32),
        ),
        in_specs=[pl.BlockSpec(memory_space=pltpu.HBM)] * 4,
        out_specs=(pl.BlockSpec(memory_space=pltpu.VMEM),) * 2,
        scratch_shapes=scratch,
        compiler_params=pltpu.CompilerParams(
            collective_id=0, has_side_effects=True, vmem_limit_bytes=VMEM_LIMIT
        ),
    )(*[pltpu.with_memory_space_constraint(x, pltpu.HBM) for x in operands])
    return (finals * scale[None]).astype(bf16).reshape(rows, classes)


def solution(mesh):
    return jax.shard_map(
        functools.partial(local, mesh.shape["vp"], mesh.shape["rep"]),
        mesh=mesh,
        in_specs=(
            P(("vp", "rep"), None),
            P(("vp", "rep"), None, None),
            P(("vp", "rep")),
            P(("vp", "rep"), None, None),
        ),
        out_specs=P(("vp", "rep"), None),
        check_vma=False,
    )
```

```python
import functools

import jax
import jax.numpy as jnp
from jax import lax
from jax.experimental import pallas as pl
from jax.experimental.pallas import tpu as pltpu
from jax.sharding import PartitionSpec as P

ITERS = 3
LANES = 128
MESH = pl.DeviceIdType.MESH
LOADS = 8
UNROLL = 64
VMEM_LIMIT = 40 * 1024 * 1024


def kernel(vp_count, rep_count, vertices, slots, halves, *refs):
    cols_hbm, rows_hbm, feat_hbm, tiles_hbm, finals_ref, scale_ref = refs[:6]
    it_refs = iter(refs[6:])
    take = lambda count: [next(it_refs) for _ in range(count)]
    tiles = take(1)[0]
    tables = [take(halves) for _ in range(ITERS)]
    feats = take(halves)
    owns = take(halves)
    sends = [take(halves) for _ in range(ITERS)]
    first = take(halves)
    second = take(halves)
    mine = take(ITERS)
    got = take(ITERS)
    relays = take(ITERS * halves - 1)
    order, place, cols_ref, rows_ref = take(4)
    (index_sem, tile_sem, feat_sem, table_sem, send_sem, recv_sem, mass_send, mass_recv, relay_send, relay_recv) = take(10)

    nblocks, tile_size = feats[0].shape[0], feats[0].shape[1]
    ntiles = tiles.shape[0]
    per_row = ntiles // nblocks
    my_vp, my_rep = lax.axis_index("vp"), lax.axis_index("rep")
    me = my_vp * rep_count + my_rep
    shards = vp_count * rep_count

    cols_load = pltpu.make_async_copy(cols_hbm, cols_ref, index_sem.at[0])
    rows_load = pltpu.make_async_copy(rows_hbm, rows_ref, index_sem.at[1])
    rows_load.start()
    cols_load.start()
    own_loads, table_loads = [], []
    for h in range(halves):
        part = feat_hbm.at[:, :, pl.ds(h * LANES, LANES)]
        own_loads.append(pltpu.make_async_copy(part, feats[h], feat_sem.at[h]))
        table_loads.append(
            pltpu.make_async_copy(part, tables[0][h].at[pl.ds(0, nblocks)], table_sem.at[h])
        )
    for h in range(halves):
        own_loads[h].start()
    for h in range(halves):
        table_loads[h].start()
    chunk = ntiles // LOADS
    tile_loads = []
    for k in range(LOADS):
        piece = pl.ds(k * chunk, chunk)
        tile_loads.append(pltpu.make_async_copy(tiles_hbm.at[piece], tiles.at[piece], tile_sem.at[k]))
        tile_loads[-1].start()

    def device_at(distance):
        flat = lax.rem(me + distance + shards, shards)
        return flat // rep_count, lax.rem(flat, rep_count)

    def peer_at(o):
        size = 1 + 3 * (o // 2)
        return device_at(size * (1 - 2 * lax.rem(o, 2)))

    barrier = pltpu.get_barrier_semaphore()

    def greet(k, carry):
        pl.semaphore_signal(barrier, inc=1, device_id=device_at(k), device_id_type=MESH)
        return carry

    lax.fori_loop(1, shards, greet, 0)

    rows_load.wait()
    cols_load.wait()

    def sent(o, j):
        return rows_ref[0, o, j]

    direct = 2 + lax.rem(me // 4, 2)
    passed = 5 - direct
    peers = (passed, direct, 0, 1)

    turns = []
    for b in range(nblocks):
        turn = jnp.int32(4)
        for g in reversed(range(4)):
            hit = sent(peers[g], 0) == b
            for j in range(1, slots):
                hit = hit | (sent(peers[g], j) == b)
            turn = jnp.where(hit, g, turn)
        turns.append(turn * nblocks + b)
    places = []
    for b in range(nblocks):
        at = jnp.int32(0)
        for c in range(nblocks):
            if c != b:
                at = at + jnp.where(turns[c] < turns[b], 1, 0)
        places.append(at)
        place[b] = at
    for b in range(4 * slots):
        place[nblocks + b] = jnp.int32(nblocks + b)
    for k in range(nblocks):
        row = jnp.int32(0)
        for b in range(nblocks):
            row = row + jnp.where(places[b] == k, b, 0)
        order[k] = row

    pl.semaphore_wait(barrier, shards - 1)

    def halo_copy(it, h, o):
        at = (it * halves + h) * 4 + o
        return pltpu.make_async_remote_copy(
            src_ref=sends[it][h].at[pl.ds(o * slots, slots)],
            dst_ref=tables[it][h].at[pl.ds(nblocks + o * slots, slots)],
            send_sem=send_sem.at[at],
            recv_sem=recv_sem.at[at],
            device_id=peer_at(o),
            device_id_type=MESH,
        )

    def fill_halo(it, h, o, source):
        for j in range(slots):
            row = rows_ref[0, o, j]
            sends[it][h][o * slots + j] = source[place[row] if it else row]

    steps = [(it, h) for it in range(ITERS) for h in range(halves)]

    def relay_copy(it, h):
        at = it * halves + h
        return pltpu.make_async_remote_copy(
            src_ref=sends[it][h].at[pl.ds(passed * slots, slots)],
            dst_ref=relays[at - 1],
            send_sem=relay_send.at[at - 1],
            recv_sem=relay_recv.at[at - 1],
            device_id=device_at(8 * (5 - 2 * passed)),
            device_id_type=MESH,
        )

    def forward_copy(it, h):
        at = it * halves + h
        return pltpu.make_async_remote_copy(
            src_ref=relays[at - 1],
            dst_ref=tables[it][h].at[pl.ds(nblocks + passed * slots, slots)],
            send_sem=send_sem.at[at * 4 + passed],
            recv_sem=recv_sem.at[at * 4 + passed],
            device_id=peer_at(direct),
            device_id_type=MESH,
        )

    def mass_copy(it, k):
        return pltpu.make_async_remote_copy(
            src_ref=mine[it],
            dst_ref=got[it].at[k - 1],
            send_sem=mass_send.at[it],
            recv_sem=mass_recv.at[it],
            device_id=device_at(k),
            device_id_type=MESH,
        )

    def mass_all(it):
        return pltpu.make_async_remote_copy(
            src_ref=got[it],
            dst_ref=got[it],
            send_sem=mass_send.at[it],
            recv_sem=mass_recv.at[it],
            device_id=device_at(1),
            device_id_type=MESH,
        )

    def mass_first(it, masses):
        mine[it][...] = jnp.concatenate(masses, axis=1)

        def one(k, carry):
            mass_copy(it, k).start()
            return carry

        lax.fori_loop(1, shards, one, 0, unroll=shards <= UNROLL)

    def mass_total(it):
        mass_all(it).wait_recv()
        total = mine[it][...] + jnp.sum(got[it][...], axis=0)
        return 1.0 / jnp.sqrt(0.05 + total / vertices)

    def half_of(gain, h):
        return gain[:, h * LANES : (h + 1) * LANES]

    def squares(blended):
        return jnp.sum((blended * blended).reshape(tile_size // 8, 8, LANES), axis=0)

    def propagate(it, h, gains=None):
        table = tables[it][h]
        last = it + 1 == ITERS

        def row(k, mass):
            r = k if last else order[k]
            first_tile = r * per_row
            slot = lambda t: cols_ref[first_tile + t]
            source = slot if it == 0 else lambda t: place[slot(t)]
            left = jnp.concatenate([tiles[first_tile + t] for t in range(per_row)], axis=1)
            right = jnp.concatenate([table[source(t)] for t in range(per_row)], axis=0)
            total = jnp.dot(left, right, preferred_element_type=jnp.float32)
            if last:
                inner = 0.729 * gains[0] * total + first[h][place[r]]
                if len(gains) == 1:
                    finals_ref[k, :, h * LANES : (h + 1) * LANES] = inner
                    return mass
                blended = gains[1] * inner + 0.1 * feats[h][r].astype(jnp.float32)
                finals_ref[k, :, h * LANES : (h + 1) * LANES] = blended
                return mass + squares(blended)
            rounded = total.astype(jnp.bfloat16)
            owns[h][k] = rounded
            tables[it + 1][h][k] = rounded
            if it:
                second[h][k] = total
                return mass
            first[h][k] = total
            return mass + squares(0.9 * total + 0.1 * feats[h][r].astype(jnp.float32))

        def group(g, mass):
            for k in range(nblocks // 4):
                mass = row(g * (nblocks // 4) + k, mass)
            if not last:
                o = jnp.where(g == 0, passed, jnp.where(g == 1, direct, g - 2))
                fill_halo(it + 1, h, o, owns[h])

                @pl.when(g == 0)
                def _():
                    relay_copy(it + 1, h).start()

                @pl.when(g > 0)
                def _():
                    halo_copy(it + 1, h, o).start()

            return mass

        mass = lax.fori_loop(0, 4, group, jnp.zeros((8, LANES), jnp.float32))
        return jnp.sum(mass, axis=0, keepdims=True)

    def blend_second(h, g1):
        def row(k, mass):
            one, two = first[h][k], second[h][k]
            feat = feats[h][order[k]].astype(jnp.float32)
            first[h][k] = 0.09 * (0.9 * g1 * two + one)
            return mass + squares(0.9 * g1 * (0.9 * two + 0.1 * one) + 0.1 * feat)

        mass = lax.fori_loop(0, nblocks, row, jnp.zeros((8, LANES), jnp.float32), unroll=4)
        return jnp.sum(mass, axis=0, keepdims=True)

    def blend_third(h, g2):
        def row(k, mass):
            inner = finals_ref[k, :, h * LANES : (h + 1) * LANES]
            blended = g2 * inner + 0.1 * feats[h][k].astype(jnp.float32)
            finals_ref[k, :, h * LANES : (h + 1) * LANES] = blended
            return mass + squares(blended)

        mass = lax.fori_loop(0, nblocks, row, jnp.zeros((8, LANES), jnp.float32), unroll=4)
        return jnp.sum(mass, axis=0, keepdims=True)

    for h in range(halves):
        own_loads[h].wait()
        for o in peers:
            fill_halo(0, h, o, feats[h])
        if h:
            relay_copy(0, h).start()
        for o in peers[1:] if h else peers:
            halo_copy(0, h, o).start()
    for h in range(halves):
        table_loads[h].wait()
    for load in tile_loads:
        load.wait()

    def halos(it, h):
        for o in range(4):
            halo_copy(it, h, o).wait_recv()

    masses, g1 = [], None
    for at, (it, h) in enumerate(steps):
        if at + 1 < len(steps):
            relay_copy(*steps[at + 1]).wait_recv()
            forward_copy(*steps[at + 1]).start()
        halos(it, h)
        final = h + 1 == halves
        if it == 0:
            masses.append(propagate(0, h))
        elif it == 1:
            propagate(1, h)
        elif not final:
            propagate(2, h, (half_of(g1, h),))
        else:
            g2 = mass_total(1)
            masses = [blend_third(other, half_of(g2, other)) for other in range(h)]
            masses.append(propagate(2, h, (half_of(g1, h), half_of(g2, h))))
        if it == 0 and final:
            mass_first(0, masses)
        if it == 1 and final:
            g1 = mass_total(0)
            mass_first(1, [blend_second(each, half_of(g1, each)) for each in range(halves)])
    for at, step in enumerate(steps):
        for o in peers[1:]:
            halo_copy(*step, o).wait_send()
        if at:
            relay_copy(*step).wait_send()
            forward_copy(*step).wait_send()
        else:
            halo_copy(*step, passed).wait_send()
    mass_first(2, masses)
    scale_ref[...] = mass_total(2)
    for it in range(ITERS):
        mass_all(it).wait_send()


def local(vp_count, rep_count, features, tile_values, tile_cols, halo_rows):
    tile_size = tile_values.shape[1]
    rows, classes = features.shape
    nblocks = rows // tile_size
    slots = halo_rows.shape[2]
    halves = classes // LANES
    shards = vp_count * rep_count
    block = (tile_size, LANES)
    bf16, f32 = jnp.bfloat16, jnp.float32
    each = ITERS * halves
    scratch = [pltpu.VMEM(tile_values.shape, bf16)]
    scratch += [pltpu.VMEM((nblocks + 4 * slots,) + block, bf16)] * each
    scratch += [pltpu.VMEM((nblocks,) + block, bf16)] * (2 * halves)
    scratch += [pltpu.VMEM((4 * slots,) + block, bf16)] * each
    scratch += [pltpu.VMEM((nblocks,) + block, f32)] * (2 * halves)
    scratch += [pltpu.VMEM((1, classes), f32)] * ITERS
    scratch += [pltpu.VMEM((shards - 1, 1, classes), f32)] * ITERS
    scratch += [pltpu.VMEM((slots,) + block, bf16)] * (each - 1)
    scratch += [pltpu.SMEM((nblocks,), jnp.int32), pltpu.SMEM((nblocks + 4 * slots,), jnp.int32)]
    scratch += [pltpu.SMEM(tile_cols.shape, jnp.int32), pltpu.SMEM(halo_rows.shape, jnp.int32)]
    dma = lambda *shape: pltpu.SemaphoreType.DMA(shape)
    scratch += [dma(2), dma(LOADS), dma(halves), dma(halves), dma(each * 4), dma(each * 4)]
    scratch += [dma(ITERS)] * 2
    scratch += [dma(each - 1)] * 2
    operands = (tile_cols, halo_rows, features.reshape(nblocks, tile_size, classes), tile_values)
    finals, scale = pl.pallas_call(
        functools.partial(kernel, vp_count, rep_count, rows * shards, slots, halves),
        out_shape=(
            pltpu.VMEM((nblocks, tile_size, classes), f32),
            pltpu.VMEM((1, classes), f32),
        ),
        in_specs=[pl.BlockSpec(memory_space=pltpu.HBM)] * 4,
        out_specs=(pl.BlockSpec(memory_space=pltpu.VMEM),) * 2,
        scratch_shapes=scratch,
        compiler_params=pltpu.CompilerParams(
            collective_id=0, has_side_effects=True, vmem_limit_bytes=VMEM_LIMIT
        ),
    )(*[pltpu.with_memory_space_constraint(x, pltpu.HBM) for x in operands])
    return (finals * scale[None]).astype(bf16).reshape(rows, classes)


def solution(mesh):
    return jax.shard_map(
        functools.partial(local, mesh.shape["vp"], mesh.shape["rep"]),
        mesh=mesh,
        in_specs=(
            P(("vp", "rep"), None),
            P(("vp", "rep"), None, None),
            P(("vp", "rep")),
            P(("vp", "rep"), None, None),
        ),
        out_specs=P(("vp", "rep"), None),
        check_vma=False,
    )
```

```python
import functools

import jax
import jax.numpy as jnp
from jax import lax
from jax.experimental import pallas as pl
from jax.experimental.pallas import tpu as pltpu
from jax.sharding import PartitionSpec as P

ITERS = 3
LANES = 128
MESH = pl.DeviceIdType.MESH
LOADS = 8
LATE = 4
UNROLL = 64
VMEM_LIMIT = 40 * 1024 * 1024


def kernel(vp_count, rep_count, vertices, slots, halves, *refs):
    cols_hbm, rows_hbm, feat_hbm, tiles_hbm, finals_ref, scale_ref = refs[:6]
    it_refs = iter(refs[6:])
    take = lambda count: [next(it_refs) for _ in range(count)]
    tiles = take(1)[0]
    tables = [take(halves) for _ in range(ITERS)]
    feats = take(halves)
    owns = take(halves)
    sends = [take(halves) for _ in range(ITERS)]
    first = take(halves)
    second = take(halves)
    mine = take(ITERS)
    got = take(ITERS)
    relays = take(ITERS * halves - 1)
    late, dense = take(2)
    order, place, cols_ref, rows_ref = take(4)
    (index_sem, tile_sem, feat_sem, table_sem, send_sem, recv_sem, mass_send, mass_recv, relay_send, relay_recv) = take(10)

    nblocks, tile_size = feats[0].shape[0], feats[0].shape[1]
    ntiles = tiles.shape[0]
    per_row = ntiles // nblocks
    my_vp, my_rep = lax.axis_index("vp"), lax.axis_index("rep")
    me = my_vp * rep_count + my_rep
    shards = vp_count * rep_count

    cols_load = pltpu.make_async_copy(cols_hbm, cols_ref, index_sem.at[0])
    rows_load = pltpu.make_async_copy(rows_hbm, rows_ref, index_sem.at[1])
    rows_load.start()
    cols_load.start()
    own_loads, table_loads = [], []
    for h in range(halves):
        part = feat_hbm.at[:, :, pl.ds(h * LANES, LANES)]
        own_loads.append(pltpu.make_async_copy(part, feats[h], feat_sem.at[h]))
        table_loads.append(
            pltpu.make_async_copy(part, tables[0][h].at[pl.ds(0, nblocks)], table_sem.at[h])
        )
    for h in range(halves):
        own_loads[h].start()
    for h in range(halves):
        table_loads[h].start()
    chunk = ntiles // LOADS
    tile_loads = []
    for k in range(LOADS):
        piece = pl.ds(k * chunk, chunk)
        tile_loads.append(pltpu.make_async_copy(tiles_hbm.at[piece], tiles.at[piece], tile_sem.at[k]))
        tile_loads[-1].start()

    def device_at(distance):
        flat = lax.rem(me + distance + shards, shards)
        return flat // rep_count, lax.rem(flat, rep_count)

    def peer_at(o):
        size = 1 + 3 * (o // 2)
        return device_at(size * (1 - 2 * lax.rem(o, 2)))

    barrier = pltpu.get_barrier_semaphore()

    def greet(k, carry):
        pl.semaphore_signal(barrier, inc=1, device_id=device_at(k), device_id_type=MESH)
        return carry

    lax.fori_loop(1, shards, greet, 0)

    rows_load.wait()
    cols_load.wait()

    def sent(o, j):
        return rows_ref[0, o, j]

    direct = 2 + lax.rem(me // 4, 2)
    passed = 5 - direct
    peers = (passed, direct, 0, 1)

    turns = []
    for b in range(nblocks):
        turn = jnp.int32(4)
        for g in reversed(range(4)):
            hit = sent(peers[g], 0) == b
            for j in range(1, slots):
                hit = hit | (sent(peers[g], j) == b)
            turn = jnp.where(hit, g, turn)
        turns.append(turn * nblocks + b)
    places = []
    for b in range(nblocks):
        at = jnp.int32(0)
        for c in range(nblocks):
            if c != b:
                at = at + jnp.where(turns[c] < turns[b], 1, 0)
        places.append(at)
        place[b] = at
    for b in range(4 * slots):
        place[nblocks + b] = jnp.int32(nblocks + b)
    for k in range(nblocks):
        row = jnp.int32(0)
        for b in range(nblocks):
            row = row + jnp.where(places[b] == k, b, 0)
        order[k] = row

    pl.semaphore_wait(barrier, shards - 1)

    def halo_copy(it, h, o):
        at = (it * halves + h) * 4 + o
        return pltpu.make_async_remote_copy(
            src_ref=sends[it][h].at[pl.ds(o * slots, slots)],
            dst_ref=tables[it][h].at[pl.ds(nblocks + o * slots, slots)],
            send_sem=send_sem.at[at],
            recv_sem=recv_sem.at[at],
            device_id=peer_at(o),
            device_id_type=MESH,
        )

    def fill_halo(it, h, o, source):
        for j in range(slots):
            row = rows_ref[0, o, j]
            sends[it][h][o * slots + j] = source[place[row] if it else row]

    steps = [(it, h) for it in range(ITERS) for h in range(halves)]

    def relay_copy(it, h):
        at = it * halves + h
        return pltpu.make_async_remote_copy(
            src_ref=sends[it][h].at[pl.ds(passed * slots, slots)],
            dst_ref=relays[at - 1],
            send_sem=relay_send.at[at - 1],
            recv_sem=relay_recv.at[at - 1],
            device_id=device_at(8 * (5 - 2 * passed)),
            device_id_type=MESH,
        )

    def forward_copy(it, h):
        at = it * halves + h
        table = tables[it][h].at[pl.ds(nblocks + passed * slots, slots)]
        return pltpu.make_async_remote_copy(
            src_ref=relays[at - 1],
            dst_ref=late if at + 1 == len(steps) else table,
            send_sem=send_sem.at[at * 4 + passed],
            recv_sem=recv_sem.at[at * 4 + passed],
            device_id=peer_at(direct),
            device_id_type=MESH,
        )

    def mass_copy(it, k):
        return pltpu.make_async_remote_copy(
            src_ref=mine[it],
            dst_ref=got[it].at[k - 1],
            send_sem=mass_send.at[it],
            recv_sem=mass_recv.at[it],
            device_id=device_at(k),
            device_id_type=MESH,
        )

    def mass_all(it):
        return pltpu.make_async_remote_copy(
            src_ref=got[it],
            dst_ref=got[it],
            send_sem=mass_send.at[it],
            recv_sem=mass_recv.at[it],
            device_id=device_at(1),
            device_id_type=MESH,
        )

    def mass_first(it, masses):
        mine[it][...] = jnp.concatenate(masses, axis=1)

        def one(k, carry):
            mass_copy(it, k).start()
            return carry

        lax.fori_loop(1, shards, one, 0, unroll=shards <= UNROLL)

    def mass_total(it):
        mass_all(it).wait_recv()
        total = mine[it][...] + jnp.sum(got[it][...], axis=0)
        return 1.0 / jnp.sqrt(0.05 + total / vertices)

    def half_of(gain, h):
        return gain[:, h * LANES : (h + 1) * LANES]

    def squares(blended):
        return jnp.sum((blended * blended).reshape(tile_size // 8, 8, LANES), axis=0)

    def propagate(it, h, g1=None, g2=None):
        table = tables[it][h]
        last = it + 1 == ITERS

        def row(k, mass):
            r = k if last else order[k]
            first_tile = r * per_row
            slot = lambda t: cols_ref[first_tile + t]
            source = slot if it == 0 else lambda t: place[slot(t)]
            left = jnp.concatenate([tiles[first_tile + t] for t in range(per_row)], axis=1)
            right = jnp.concatenate([table[source(t)] for t in range(per_row)], axis=0)
            total = jnp.dot(left, right, preferred_element_type=jnp.float32)
            if last:
                finals_ref[k, :, h * LANES : (h + 1) * LANES] = 0.729 * g1 * total + first[h][place[r]]
                if g2 is None:
                    return mass
                return tuple(
                    part + squares(blend_third(other, k, half_of(g2, other), 0.0))
                    for other, part in enumerate(mass)
                )
            rounded = total.astype(jnp.bfloat16)
            owns[h][k] = rounded
            tables[it + 1][h][k] = rounded
            if it:
                second[h][k] = total
                return mass
            first[h][k] = total
            return mass + squares(0.9 * total + 0.1 * feats[h][r].astype(jnp.float32))

        def group(g, mass):
            for k in range(nblocks // 4):
                mass = row(g * (nblocks // 4) + k, mass)
            if not last:
                o = jnp.where(g == 0, passed, jnp.where(g == 1, direct, g - 2))
                fill_halo(it + 1, h, o, owns[h])

                @pl.when(g == 0)
                def _():
                    relay_copy(it + 1, h).start()

                @pl.when(g > 0)
                def _():
                    halo_copy(it + 1, h, o).start()

            return mass

        none = jnp.zeros((8, LANES), jnp.float32)
        mass = lax.fori_loop(0, 4, group, none if g2 is None else (none,) * h, unroll=4)
        return jax.tree.map(lambda part: jnp.sum(part, axis=0, keepdims=True), mass)

    def blend_second(h, g1):
        def row(k, mass):
            one, two = first[h][k], second[h][k]
            feat = feats[h][order[k]].astype(jnp.float32)
            first[h][k] = 0.09 * (0.9 * g1 * two + one)
            return mass + squares(0.9 * g1 * (0.9 * two + 0.1 * one) + 0.1 * feat)

        mass = lax.fori_loop(0, nblocks, row, jnp.zeros((8, LANES), jnp.float32), unroll=4)
        return jnp.sum(mass, axis=0, keepdims=True)

    def blend_third(h, k, g2, more):
        inner = finals_ref[k, :, h * LANES : (h + 1) * LANES] + more
        blended = g2 * inner + 0.1 * feats[h][k].astype(jnp.float32)
        finals_ref[k, :, h * LANES : (h + 1) * LANES] = blended
        return blended

    def gather_late():
        part = tile_size // 4

        def row(r, carry):
            for p in range(4):
                sums = [jnp.zeros((part, tile_size), jnp.float32)] * slots
                for t in range(per_row):
                    tile = tiles[r * per_row + t, p * part : (p + 1) * part].astype(jnp.float32)
                    slot = cols_ref[r * per_row + t] - nblocks - direct * slots
                    sums = [total + jnp.where(slot == j, tile, 0.0) for j, total in enumerate(sums)]
                for j, total in enumerate(sums):
                    columns = slice(j * tile_size, (j + 1) * tile_size)
                    dense[r, p * part : (p + 1) * part, columns] = total.astype(jnp.bfloat16)
            return carry

        lax.fori_loop(0, nblocks, row, 0)

    def late_wait():
        at = len(steps) - 1
        pltpu.make_async_remote_copy(
            src_ref=late,
            dst_ref=late,
            send_sem=send_sem.at[at * 4 + direct],
            recv_sem=recv_sem.at[at * 4 + direct],
            device_id=peer_at(direct),
            device_id_type=MESH,
        ).wait_recv()

    def propagate_late(h, g1, g2):
        right = late[...].reshape(slots * tile_size, LANES)
        count = nblocks // LATE

        def group(g, mass):
            left = dense[pl.ds(g * count, count)].reshape(count * tile_size, slots * tile_size)
            total = jnp.dot(left, right, preferred_element_type=jnp.float32)
            for k in range(count):
                more = 0.729 * g1 * total[k * tile_size : (k + 1) * tile_size]
                mass = mass + squares(blend_third(h, g * count + k, g2, more))
            return mass

        mass = lax.fori_loop(0, LATE, group, jnp.zeros((8, LANES), jnp.float32), unroll=LATE)
        return jnp.sum(mass, axis=0, keepdims=True)

    for h in range(halves):
        own_loads[h].wait()
        for o in peers:
            fill_halo(0, h, o, feats[h])
        if h:
            relay_copy(0, h).start()
        for o in peers[1:] if h else peers:
            halo_copy(0, h, o).start()
    for h in range(halves):
        table_loads[h].wait()
    for load in tile_loads:
        load.wait()
    tables[-1][-1][pl.ds(nblocks + direct * slots, slots)] = jnp.zeros(late.shape, jnp.bfloat16)

    def halos(it, h):
        for o in (0, 1, passed, direct):
            if o is not direct or (it, h) != steps[-1]:
                halo_copy(it, h, o).wait_recv()

    gather_late()
    masses, g1 = [], None
    for at, (it, h) in enumerate(steps):
        if at + 1 < len(steps):
            relay_copy(*steps[at + 1]).wait_recv()
            forward_copy(*steps[at + 1]).start()
        halos(it, h)
        final = h + 1 == halves
        if it == 0:
            masses.append(propagate(0, h))
        elif it == 1:
            propagate(1, h)
        elif not final:
            propagate(2, h, half_of(g1, h))
        else:
            g2 = mass_total(1)
            masses = list(propagate(2, h, half_of(g1, h), g2))
            late_wait()
            masses.append(propagate_late(h, half_of(g1, h), half_of(g2, h)))
        if it == 0 and final:
            mass_first(0, masses)
        if it == 1 and final:
            g1 = mass_total(0)
            mass_first(1, [blend_second(each, half_of(g1, each)) for each in range(halves)])
    for at, step in enumerate(steps):
        for o in peers[1:]:
            halo_copy(*step, o).wait_send()
        if at:
            relay_copy(*step).wait_send()
            forward_copy(*step).wait_send()
        else:
            halo_copy(*step, passed).wait_send()
    mass_first(2, masses)
    scale_ref[...] = mass_total(2)
    for it in range(ITERS):
        mass_all(it).wait_send()


def local(vp_count, rep_count, features, tile_values, tile_cols, halo_rows):
    tile_size = tile_values.shape[1]
    rows, classes = features.shape
    nblocks = rows // tile_size
    slots = halo_rows.shape[2]
    halves = classes // LANES
    shards = vp_count * rep_count
    block = (tile_size, LANES)
    bf16, f32 = jnp.bfloat16, jnp.float32
    each = ITERS * halves
    scratch = [pltpu.VMEM(tile_values.shape, bf16)]
    scratch += [pltpu.VMEM((nblocks + 4 * slots,) + block, bf16)] * each
    scratch += [pltpu.VMEM((nblocks,) + block, bf16)] * (2 * halves)
    scratch += [pltpu.VMEM((4 * slots,) + block, bf16)] * each
    scratch += [pltpu.VMEM((nblocks,) + block, f32)] * (2 * halves)
    scratch += [pltpu.VMEM((1, classes), f32)] * ITERS
    scratch += [pltpu.VMEM((shards - 1, 1, classes), f32)] * ITERS
    scratch += [pltpu.VMEM((slots,) + block, bf16)] * each
    scratch += [pltpu.VMEM((nblocks, tile_size, slots * tile_size), bf16)]
    scratch += [pltpu.SMEM((nblocks,), jnp.int32), pltpu.SMEM((nblocks + 4 * slots,), jnp.int32)]
    scratch += [pltpu.SMEM(tile_cols.shape, jnp.int32), pltpu.SMEM(halo_rows.shape, jnp.int32)]
    dma = lambda *shape: pltpu.SemaphoreType.DMA(shape)
    scratch += [dma(2), dma(LOADS), dma(halves), dma(halves), dma(each * 4), dma(each * 4)]
    scratch += [dma(ITERS)] * 2
    scratch += [dma(each - 1)] * 2
    operands = (tile_cols, halo_rows, features.reshape(nblocks, tile_size, classes), tile_values)
    finals, scale = pl.pallas_call(
        functools.partial(kernel, vp_count, rep_count, rows * shards, slots, halves),
        out_shape=(
            pltpu.VMEM((nblocks, tile_size, classes), f32),
            pltpu.VMEM((1, classes), f32),
        ),
        in_specs=[pl.BlockSpec(memory_space=pltpu.HBM)] * 4,
        out_specs=(pl.BlockSpec(memory_space=pltpu.VMEM),) * 2,
        scratch_shapes=scratch,
        compiler_params=pltpu.CompilerParams(
            collective_id=0, has_side_effects=True, vmem_limit_bytes=VMEM_LIMIT
        ),
    )(*[pltpu.with_memory_space_constraint(x, pltpu.HBM) for x in operands])
    return (finals * scale[None]).astype(bf16).reshape(rows, classes)


def solution(mesh):
    return jax.shard_map(
        functools.partial(local, mesh.shape["vp"], mesh.shape["rep"]),
        mesh=mesh,
        in_specs=(
            P(("vp", "rep"), None),
            P(("vp", "rep"), None, None),
            P(("vp", "rep")),
            P(("vp", "rep"), None, None),
        ),
        out_specs=P(("vp", "rep"), None),
        check_vma=False,
    )
```

```python
import functools

import jax
import jax.numpy as jnp
from jax import lax
from jax.experimental import pallas as pl
from jax.experimental.pallas import tpu as pltpu
from jax.sharding import PartitionSpec as P

ITERS = 3
LANES = 128
MESH = pl.DeviceIdType.MESH
LOADS = 8
LATE = 4
UNROLL = 64
VMEM_LIMIT = 40 * 1024 * 1024


def kernel(vp_count, rep_count, vertices, slots, halves, *refs):
    cols_hbm, rows_hbm, feat_hbm, tiles_hbm, finals_ref, scale_ref = refs[:6]
    it_refs = iter(refs[6:])
    take = lambda count: [next(it_refs) for _ in range(count)]
    tiles = take(1)[0]
    tables = [take(halves) for _ in range(ITERS)]
    feats = take(halves)
    owns = take(halves)
    sends = [take(halves) for _ in range(ITERS)]
    first = take(halves)
    second = take(halves)
    mine, got = take(2)
    relays = take(ITERS * halves - 1)
    late, dense = take(2)
    order, place, cols_ref, rows_ref = take(4)
    index_sem, tile_sem, feat_sem, table_sem, send_sem, recv_sem, mass_send, mass_recv, relay_recv = take(9)

    nblocks, tile_size = feats[0].shape[0], feats[0].shape[1]
    ntiles = tiles.shape[0]
    per_row = ntiles // nblocks
    my_vp, my_rep = lax.axis_index("vp"), lax.axis_index("rep")
    me = my_vp * rep_count + my_rep
    shards = vp_count * rep_count

    cols_load = pltpu.make_async_copy(cols_hbm, cols_ref, index_sem.at[0])
    rows_load = pltpu.make_async_copy(rows_hbm, rows_ref, index_sem.at[1])
    rows_load.start()
    cols_load.start()
    own_loads, table_loads = [], []
    for h in range(halves):
        part = feat_hbm.at[:, :, pl.ds(h * LANES, LANES)]
        own_loads.append(pltpu.make_async_copy(part, feats[h], feat_sem.at[h]))
        table_loads.append(
            pltpu.make_async_copy(part, tables[0][h].at[pl.ds(0, nblocks)], table_sem.at[h])
        )
    for h in range(halves):
        own_loads[h].start()
    for h in range(halves):
        table_loads[h].start()
    chunk = ntiles // LOADS
    for k in range(LOADS):
        piece = pl.ds(k * chunk, chunk)
        pltpu.make_async_copy(tiles_hbm.at[piece], tiles.at[piece], tile_sem.at[0]).start()

    def device_at(distance):
        flat = lax.rem(me + distance + shards, shards)
        return flat // rep_count, lax.rem(flat, rep_count)

    def peer_at(o):
        size = 1 + 3 * (o // 2)
        return device_at(size * (1 - 2 * lax.rem(o, 2)))

    barrier = pltpu.get_barrier_semaphore()

    def greet(k, carry):
        pl.semaphore_signal(barrier, inc=1, device_id=device_at(k), device_id_type=MESH)
        return carry

    lax.fori_loop(1, shards, greet, 0)

    rows_load.wait()
    cols_load.wait()

    def sent(o, j):
        return rows_ref[0, o, j]

    direct = 2 + lax.rem(me // 4, 2)
    passed = 5 - direct
    peers = (passed, direct, 0, 1)

    turns = []
    for b in range(nblocks):
        turn = jnp.int32(4)
        for g in reversed(range(4)):
            hit = sent(peers[g], 0) == b
            for j in range(1, slots):
                hit = hit | (sent(peers[g], j) == b)
            turn = jnp.where(hit, g, turn)
        turns.append(turn * nblocks + b)
    places = []
    for b in range(nblocks):
        at = jnp.int32(0)
        for c in range(nblocks):
            if c != b:
                at = at + jnp.where(turns[c] < turns[b], 1, 0)
        places.append(at)
        place[b] = at
    for b in range(4 * slots):
        place[nblocks + b] = jnp.int32(nblocks + b)
    for k in range(nblocks):
        row = jnp.int32(0)
        for b in range(nblocks):
            row = row + jnp.where(places[b] == k, b, 0)
        order[k] = row

    pl.semaphore_wait(barrier, shards - 1)

    def halo_copy(it, h, o):
        at = (it * halves + h) * 4 + o
        return pltpu.make_async_remote_copy(
            src_ref=sends[it][h].at[pl.ds(o * slots, slots)],
            dst_ref=tables[it][h].at[pl.ds(nblocks + o * slots, slots)],
            send_sem=send_sem.at[0],
            recv_sem=recv_sem.at[it * halves + h],
            device_id=peer_at(o),
            device_id_type=MESH,
        )

    def fill_halo(it, h, o, source):
        for j in range(slots):
            row = rows_ref[0, o, j]
            sends[it][h][o * slots + j] = source[place[row] if it else row]

    steps = [(it, h) for it in range(ITERS) for h in range(halves)]

    def relay_copy(it, h):
        at = it * halves + h
        return pltpu.make_async_remote_copy(
            src_ref=sends[it][h].at[pl.ds(passed * slots, slots)],
            dst_ref=relays[at - 1],
            send_sem=send_sem.at[0],
            recv_sem=relay_recv.at[at - 1],
            device_id=device_at(8 * (5 - 2 * passed)),
            device_id_type=MESH,
        )

    def forward_copy(it, h):
        at = it * halves + h
        table = tables[it][h].at[pl.ds(nblocks + passed * slots, slots)]
        return pltpu.make_async_remote_copy(
            src_ref=relays[at - 1],
            dst_ref=late if at + 1 == len(steps) else table,
            send_sem=send_sem.at[0],
            recv_sem=recv_sem.at[at + 1 if at + 1 == len(steps) else at],
            device_id=peer_at(direct),
            device_id_type=MESH,
        )

    def mass_copy(it, k):
        return pltpu.make_async_remote_copy(
            src_ref=mine.at[it],
            dst_ref=got.at[it, k - 1],
            send_sem=mass_send.at[0],
            recv_sem=mass_recv.at[it],
            device_id=device_at(k),
            device_id_type=MESH,
        )

    def bytes_of(ref, send, recv):
        return pltpu.make_async_remote_copy(
            src_ref=ref,
            dst_ref=ref,
            send_sem=send,
            recv_sem=recv,
            device_id=device_at(1),
            device_id_type=MESH,
        )

    def mass_first(it, masses):
        mine[it] = jnp.concatenate(masses, axis=1)

        def one(k, carry):
            mass_copy(it, k).start()
            return carry

        lax.fori_loop(1, shards, one, 0, unroll=shards <= UNROLL)

    def mass_total(it):
        bytes_of(got.at[it], mass_send.at[0], mass_recv.at[it]).wait_recv()
        total = mine[it] + jnp.sum(got[it], axis=0)
        return 1.0 / jnp.sqrt(0.05 + total / vertices)

    def half_of(gain, h):
        return gain[:, h * LANES : (h + 1) * LANES]

    def squares(blended):
        return jnp.sum((blended * blended).reshape(tile_size // 8, 8, LANES), axis=0)

    def propagate(it, h, g1=None, g2=None):
        table = tables[it][h]
        last = it + 1 == ITERS

        def row(k, mass):
            r = k if last else order[k]
            first_tile = r * per_row
            slot = lambda t: cols_ref[first_tile + t]
            source = slot if it == 0 else lambda t: place[slot(t)]
            left = jnp.concatenate([tiles[first_tile + t] for t in range(per_row)], axis=1)
            right = jnp.concatenate([table[source(t)] for t in range(per_row)], axis=0)
            total = jnp.dot(left, right, preferred_element_type=jnp.float32)
            if last:
                finals_ref[k, :, h * LANES : (h + 1) * LANES] = 0.729 * g1 * total + first[h][place[r]]
                if g2 is None:
                    return mass
                return tuple(
                    part + squares(blend_third(other, k, half_of(g2, other), 0.0))
                    for other, part in enumerate(mass)
                )
            rounded = total.astype(jnp.bfloat16)
            owns[h][k] = rounded
            tables[it + 1][h][k] = rounded
            if it:
                second[h][k] = total
                return mass
            first[h][k] = total
            return mass + squares(0.9 * total + 0.1 * feats[h][r].astype(jnp.float32))

        def group(g, mass):
            for k in range(nblocks // 4):
                mass = row(g * (nblocks // 4) + k, mass)
            if not last:
                o = jnp.where(g == 0, passed, jnp.where(g == 1, direct, g - 2))
                fill_halo(it + 1, h, o, owns[h])

                @pl.when(g == 0)
                def _():
                    relay_copy(it + 1, h).start()

                @pl.when(g > 0)
                def _():
                    halo_copy(it + 1, h, o).start()

            return mass

        none = jnp.zeros((8, LANES), jnp.float32)
        mass = lax.fori_loop(0, 4, group, none if g2 is None else (none,) * h, unroll=2)
        return jax.tree.map(lambda part: jnp.sum(part, axis=0, keepdims=True), mass)

    def blend_second(h, g1):
        def row(k, mass):
            one, two = first[h][k], second[h][k]
            feat = feats[h][order[k]].astype(jnp.float32)
            first[h][k] = 0.09 * (0.9 * g1 * two + one)
            return mass + squares(0.9 * g1 * (0.9 * two + 0.1 * one) + 0.1 * feat)

        mass = lax.fori_loop(0, nblocks, row, jnp.zeros((8, LANES), jnp.float32), unroll=4)
        return jnp.sum(mass, axis=0, keepdims=True)

    def blend_third(h, k, g2, more):
        inner = finals_ref[k, :, h * LANES : (h + 1) * LANES] + more
        blended = g2 * inner + 0.1 * feats[h][k].astype(jnp.float32)
        finals_ref[k, :, h * LANES : (h + 1) * LANES] = blended
        return blended

    def gather_late():
        part = tile_size // 4

        def row(r, carry):
            for p in range(4):
                sums = [jnp.zeros((part, tile_size), jnp.float32)] * slots
                for t in range(per_row):
                    tile = tiles[r * per_row + t, p * part : (p + 1) * part].astype(jnp.float32)
                    slot = cols_ref[r * per_row + t] - nblocks - direct * slots
                    sums = [total + jnp.where(slot == j, tile, 0.0) for j, total in enumerate(sums)]
                for j, total in enumerate(sums):
                    columns = slice(j * tile_size, (j + 1) * tile_size)
                    dense[r, p * part : (p + 1) * part, columns] = total.astype(jnp.bfloat16)
            return carry

        lax.fori_loop(0, nblocks, row, 0)

    def propagate_late(h, g1, g2):
        right = late[...].reshape(slots * tile_size, LANES)
        count = nblocks // LATE

        def group(g, mass):
            left = dense[pl.ds(g * count, count)].reshape(count * tile_size, slots * tile_size)
            total = jnp.dot(left, right, preferred_element_type=jnp.float32)
            for k in range(count):
                more = 0.729 * g1 * total[k * tile_size : (k + 1) * tile_size]
                mass = mass + squares(blend_third(h, g * count + k, g2, more))
            return mass

        mass = lax.fori_loop(0, LATE, group, jnp.zeros((8, LANES), jnp.float32), unroll=LATE)
        return jnp.sum(mass, axis=0, keepdims=True)

    for h in range(halves):
        own_loads[h].wait()
        for o in peers:
            fill_halo(0, h, o, feats[h])
        if h:
            relay_copy(0, h).start()
        for o in peers[1:] if h else peers:
            halo_copy(0, h, o).start()
    for h in range(halves):
        table_loads[h].wait()
    pltpu.make_async_copy(tiles_hbm, tiles, tile_sem.at[0]).wait()
    tables[-1][-1][pl.ds(nblocks + direct * slots, slots)] = jnp.zeros(late.shape, jnp.bfloat16)

    def halos(at):
        it, h = steps[at]
        flows = 3 if at + 1 == len(steps) else 4
        landed = tables[it][h].at[pl.ds(nblocks, flows * slots)]
        bytes_of(landed, send_sem.at[0], recv_sem.at[at]).wait_recv()

    gather_late()
    masses, g1 = [], None
    for at, (it, h) in enumerate(steps):
        if at + 1 < len(steps):
            relay_copy(*steps[at + 1]).wait_recv()
            forward_copy(*steps[at + 1]).start()
        halos(at)
        final = h + 1 == halves
        if it == 0:
            masses.append(propagate(0, h))
        elif it == 1:
            propagate(1, h)
        elif not final:
            propagate(2, h, half_of(g1, h))
        else:
            g2 = mass_total(1)
            masses = list(propagate(2, h, half_of(g1, h), g2))
            bytes_of(late, send_sem.at[0], recv_sem.at[at + 1]).wait_recv()
            masses.append(propagate_late(h, half_of(g1, h), half_of(g2, h)))
        if it == 0 and final:
            mass_first(0, masses)
        if it == 1 and final:
            g1 = mass_total(0)
            mass_first(1, [blend_second(each, half_of(g1, each)) for each in range(halves)])
    mass_first(2, masses)
    bytes_of(tiles.at[pl.ds(0, (5 * len(steps) - 1) * slots)], send_sem.at[0], recv_sem.at[0]).wait_send()
    bytes_of(got, mass_send.at[0], mass_recv.at[0]).wait_send()
    scale_ref[...] = mass_total(2)


def local(vp_count, rep_count, features, tile_values, tile_cols, halo_rows):
    tile_size = tile_values.shape[1]
    rows, classes = features.shape
    nblocks = rows // tile_size
    slots = halo_rows.shape[2]
    halves = classes // LANES
    shards = vp_count * rep_count
    block = (tile_size, LANES)
    bf16, f32 = jnp.bfloat16, jnp.float32
    each = ITERS * halves
    scratch = [pltpu.VMEM(tile_values.shape, bf16)]
    scratch += [pltpu.VMEM((nblocks + 4 * slots,) + block, bf16)] * each
    scratch += [pltpu.VMEM((nblocks,) + block, bf16)] * (2 * halves)
    scratch += [pltpu.VMEM((4 * slots,) + block, bf16)] * each
    scratch += [pltpu.VMEM((nblocks,) + block, f32)] * (2 * halves)
    scratch += [pltpu.VMEM((ITERS, 1, classes), f32), pltpu.VMEM((ITERS, shards - 1, 1, classes), f32)]
    scratch += [pltpu.VMEM((slots,) + block, bf16)] * each
    scratch += [pltpu.VMEM((nblocks, tile_size, slots * tile_size), bf16)]
    scratch += [pltpu.SMEM((nblocks,), jnp.int32), pltpu.SMEM((nblocks + 4 * slots,), jnp.int32)]
    scratch += [pltpu.SMEM(tile_cols.shape, jnp.int32), pltpu.SMEM(halo_rows.shape, jnp.int32)]
    dma = lambda *shape: pltpu.SemaphoreType.DMA(shape)
    scratch += [dma(2), dma(1), dma(halves), dma(halves), dma(1), dma(each + 1)]
    scratch += [dma(1), dma(ITERS), dma(each - 1)]
    operands = (tile_cols, halo_rows, features.reshape(nblocks, tile_size, classes), tile_values)
    finals, scale = pl.pallas_call(
        functools.partial(kernel, vp_count, rep_count, rows * shards, slots, halves),
        out_shape=(
            pltpu.VMEM((nblocks, tile_size, classes), f32),
            pltpu.VMEM((1, classes), f32),
        ),
        in_specs=[pl.BlockSpec(memory_space=pltpu.HBM)] * 4,
        out_specs=(pl.BlockSpec(memory_space=pltpu.VMEM),) * 2,
        scratch_shapes=scratch,
        compiler_params=pltpu.CompilerParams(
            collective_id=0, has_side_effects=True, vmem_limit_bytes=VMEM_LIMIT
        ),
    )(*[pltpu.with_memory_space_constraint(x, pltpu.HBM) for x in operands])
    return (finals * scale[None]).astype(bf16).reshape(rows, classes)


def solution(mesh):
    return jax.shard_map(
        functools.partial(local, mesh.shape["vp"], mesh.shape["rep"]),
        mesh=mesh,
        in_specs=(
            P(("vp", "rep"), None),
            P(("vp", "rep"), None, None),
            P(("vp", "rep")),
            P(("vp", "rep"), None, None),
        ),
        out_specs=P(("vp", "rep"), None),
        check_vma=False,
    )
```

```python
import functools

import jax
import jax.numpy as jnp
from jax import lax
from jax.experimental import pallas as pl
from jax.experimental.pallas import tpu as pltpu
from jax.sharding import PartitionSpec as P

ITERS = 3
LANES = 128
MESH = pl.DeviceIdType.MESH
LOADS = 8
LATE = 4
UNROLL = 64
VMEM_LIMIT = 40 * 1024 * 1024


def kernel(vp_count, rep_count, vertices, slots, halves, *refs):
    cols_hbm, rows_hbm, feat_hbm, tiles_hbm, finals_ref, scale_ref = refs[:6]
    it_refs = iter(refs[6:])
    take = lambda count: [next(it_refs) for _ in range(count)]
    tiles = take(1)[0]
    tables = [take(halves) for _ in range(ITERS)]
    feats = take(halves)
    owns = take(halves)
    sends = [take(halves) for _ in range(ITERS)]
    first = take(halves)
    second = take(halves)
    mine, got = take(2)
    relays = take(ITERS * halves - 1)
    late, dense = take(2)
    order, place, cols_ref, rows_ref = take(4)
    index_sem, tile_sem, feat_sem, table_sem, send_sem, recv_sem, mass_send, mass_recv, relay_recv = take(9)

    nblocks, tile_size = feats[0].shape[0], feats[0].shape[1]
    ntiles = tiles.shape[0]
    per_row = ntiles // nblocks
    my_vp, my_rep = lax.axis_index("vp"), lax.axis_index("rep")
    me = my_vp * rep_count + my_rep
    shards = vp_count * rep_count

    cols_load = pltpu.make_async_copy(cols_hbm, cols_ref, index_sem.at[0])
    rows_load = pltpu.make_async_copy(rows_hbm, rows_ref, index_sem.at[1])
    rows_load.start()
    cols_load.start()
    own_loads, table_loads = [], []
    for h in range(halves):
        part = feat_hbm.at[:, :, pl.ds(h * LANES, LANES)]
        own_loads.append(pltpu.make_async_copy(part, feats[h], feat_sem.at[h]))
        table_loads.append(
            pltpu.make_async_copy(part, tables[0][h].at[pl.ds(0, nblocks)], table_sem.at[h])
        )
    for h in range(halves):
        own_loads[h].start()
    for h in range(halves):
        table_loads[h].start()
    chunk = ntiles // LOADS
    for k in range(LOADS):
        piece = pl.ds(k * chunk, chunk)
        pltpu.make_async_copy(tiles_hbm.at[piece], tiles.at[piece], tile_sem.at[0]).start()

    def device_at(distance):
        flat = lax.rem(me + distance + shards, shards)
        return flat // rep_count, lax.rem(flat, rep_count)

    def peer_at(o):
        size = 1 + 3 * (o // 2)
        return device_at(size * (1 - 2 * lax.rem(o, 2)))

    barrier = pltpu.get_barrier_semaphore()

    def greet(k, carry):
        pl.semaphore_signal(barrier, inc=1, device_id=device_at(k), device_id_type=MESH)
        return carry

    lax.fori_loop(1, shards, greet, 0)

    rows_load.wait()
    cols_load.wait()

    def sent(o, j):
        return rows_ref[0, o, j]

    direct = 2 + lax.rem(me // 4, 2)
    passed = 5 - direct
    peers = (passed, direct, 0, 1)

    turns = []
    for b in range(nblocks):
        turn = jnp.int32(4)
        for g in reversed(range(4)):
            hit = sent(peers[g], 0) == b
            for j in range(1, slots):
                hit = hit | (sent(peers[g], j) == b)
            turn = jnp.where(hit, g, turn)
        turns.append(turn * nblocks + b)
    places = []
    for b in range(nblocks):
        at = jnp.int32(0)
        for c in range(nblocks):
            if c != b:
                at = at + jnp.where(turns[c] < turns[b], 1, 0)
        places.append(at)
        place[b] = at
    for b in range(4 * slots):
        place[nblocks + b] = jnp.int32(nblocks + b)
    for k in range(nblocks):
        row = jnp.int32(0)
        for b in range(nblocks):
            row = row + jnp.where(places[b] == k, b, 0)
        order[k] = row

    pl.semaphore_wait(barrier, shards - 1)

    def halo_copy(it, h, o):
        at = (it * halves + h) * 4 + o
        return pltpu.make_async_remote_copy(
            src_ref=sends[it][h].at[pl.ds(o * slots, slots)],
            dst_ref=tables[it][h].at[pl.ds(nblocks + o * slots, slots)],
            send_sem=send_sem.at[0],
            recv_sem=recv_sem.at[it * halves + h],
            device_id=peer_at(o),
            device_id_type=MESH,
        )

    def fill_halo(it, h, o, source):
        for j in range(slots):
            row = rows_ref[0, o, j]
            sends[it][h][o * slots + j] = source[place[row] if it else row]

    steps = [(it, h) for it in range(ITERS) for h in range(halves)]

    def relay_copy(it, h):
        at = it * halves + h
        return pltpu.make_async_remote_copy(
            src_ref=sends[it][h].at[pl.ds(passed * slots, slots)],
            dst_ref=relays[at - 1],
            send_sem=send_sem.at[0],
            recv_sem=relay_recv.at[at - 1],
            device_id=device_at(8 * (5 - 2 * passed)),
            device_id_type=MESH,
        )

    def forward_copy(it, h):
        at = it * halves + h
        table = tables[it][h].at[pl.ds(nblocks + passed * slots, slots)]
        return pltpu.make_async_remote_copy(
            src_ref=relays[at - 1],
            dst_ref=late if at + 1 == len(steps) else table,
            send_sem=send_sem.at[0],
            recv_sem=recv_sem.at[at + 1 if at + 1 == len(steps) else at],
            device_id=peer_at(direct),
            device_id_type=MESH,
        )

    def mass_copy(it, k):
        return pltpu.make_async_remote_copy(
            src_ref=mine.at[it],
            dst_ref=got.at[it, k - 1],
            send_sem=mass_send.at[0],
            recv_sem=mass_recv.at[it],
            device_id=device_at(k),
            device_id_type=MESH,
        )

    def bytes_of(ref, send, recv):
        return pltpu.make_async_remote_copy(
            src_ref=ref,
            dst_ref=ref,
            send_sem=send,
            recv_sem=recv,
            device_id=device_at(1),
            device_id_type=MESH,
        )

    def mass_first(it, masses):
        mine[it] = jnp.concatenate(masses, axis=1)

        def one(k, carry):
            mass_copy(it, k).start()
            return carry

        lax.fori_loop(1, shards, one, 0, unroll=shards <= UNROLL)

    def mass_total(it):
        bytes_of(got.at[it], mass_send.at[0], mass_recv.at[it]).wait_recv()
        total = mine[it] + jnp.sum(got[it], axis=0)
        return 1.0 / jnp.sqrt(0.05 + total / vertices)

    def half_of(gain, h):
        return gain[:, h * LANES : (h + 1) * LANES]

    def squares(blended):
        return jnp.sum((blended * blended).reshape(tile_size // 8, 8, LANES), axis=0)

    def propagate(it, h, g1=None, g2=None):
        table = tables[it][h]
        last = it + 1 == ITERS

        def row(k, mass):
            r = k if last else order[k]
            first_tile = r * per_row
            slot = lambda t: cols_ref[first_tile + t]
            source = slot if it == 0 else lambda t: place[slot(t)]
            left = jnp.concatenate([tiles[first_tile + t] for t in range(per_row)], axis=1)
            right = jnp.concatenate([table[source(t)] for t in range(per_row)], axis=0)
            total = jnp.dot(left, right, preferred_element_type=jnp.float32)
            if last:
                finals_ref[k, :, h * LANES : (h + 1) * LANES] = 0.729 * g1 * total + first[h][place[r]]
                if g2 is None:
                    return mass
                return tuple(
                    part + squares(blend_third(other, k, half_of(g2, other), 0.0))
                    for other, part in enumerate(mass)
                )
            rounded = total.astype(jnp.bfloat16)
            owns[h][k] = rounded
            tables[it + 1][h][k] = rounded
            if it:
                second[h][k] = total
                return mass
            first[h][k] = total
            return mass + squares(0.9 * total + 0.1 * feats[h][r].astype(jnp.float32))

        def group(g, mass):
            for k in range(nblocks // 4):
                mass = row(g * (nblocks // 4) + k, mass)
            if not last:
                o = jnp.where(g == 0, passed, jnp.where(g == 1, direct, g - 2))
                fill_halo(it + 1, h, o, owns[h])

                @pl.when(g == 0)
                def _():
                    relay_copy(it + 1, h).start()

                @pl.when(g > 0)
                def _():
                    halo_copy(it + 1, h, o).start()

            return mass

        none = jnp.zeros((8, LANES), jnp.float32)
        mass = lax.fori_loop(0, 4, group, none if g2 is None else (none,) * h, unroll=4 if last else 2)
        return jax.tree.map(lambda part: jnp.sum(part, axis=0, keepdims=True), mass)

    def blend_second(h, g1):
        def row(k, mass):
            one, two = first[h][k], second[h][k]
            feat = feats[h][order[k]].astype(jnp.float32)
            first[h][k] = 0.09 * (0.9 * g1 * two + one)
            return mass + squares(0.9 * g1 * (0.9 * two + 0.1 * one) + 0.1 * feat)

        mass = lax.fori_loop(0, nblocks, row, jnp.zeros((8, LANES), jnp.float32), unroll=4)
        return jnp.sum(mass, axis=0, keepdims=True)

    def blend_third(h, k, g2, more):
        inner = finals_ref[k, :, h * LANES : (h + 1) * LANES] + more
        blended = g2 * inner + 0.1 * feats[h][k].astype(jnp.float32)
        finals_ref[k, :, h * LANES : (h + 1) * LANES] = blended
        return blended

    def gather_late():
        part = tile_size // 4

        def row(r, carry):
            for p in range(4):
                sums = [jnp.zeros((part, tile_size), jnp.float32)] * slots
                for t in range(per_row):
                    tile = tiles[r * per_row + t, p * part : (p + 1) * part].astype(jnp.float32)
                    slot = cols_ref[r * per_row + t] - nblocks - direct * slots
                    sums = [total + jnp.where(slot == j, tile, 0.0) for j, total in enumerate(sums)]
                for j, total in enumerate(sums):
                    columns = slice(j * tile_size, (j + 1) * tile_size)
                    dense[r, p * part : (p + 1) * part, columns] = total.astype(jnp.bfloat16)
            return carry

        lax.fori_loop(0, nblocks, row, 0)

    def propagate_late(h, g1, g2):
        right = late[...].reshape(slots * tile_size, LANES)
        count = nblocks // LATE

        def group(g, mass):
            left = dense[pl.ds(g * count, count)].reshape(count * tile_size, slots * tile_size)
            total = jnp.dot(left, right, preferred_element_type=jnp.float32)
            for k in range(count):
                more = 0.729 * g1 * total[k * tile_size : (k + 1) * tile_size]
                mass = mass + squares(blend_third(h, g * count + k, g2, more))
            return mass

        mass = lax.fori_loop(0, LATE, group, jnp.zeros((8, LANES), jnp.float32), unroll=LATE)
        return jnp.sum(mass, axis=0, keepdims=True)

    for h in range(halves):
        own_loads[h].wait()
        for o in peers:
            fill_halo(0, h, o, feats[h])
        if h:
            relay_copy(0, h).start()
        for o in peers[1:] if h else peers:
            halo_copy(0, h, o).start()
    for h in range(halves):
        table_loads[h].wait()
    pltpu.make_async_copy(tiles_hbm, tiles, tile_sem.at[0]).wait()
    tables[-1][-1][pl.ds(nblocks + direct * slots, slots)] = jnp.zeros(late.shape, jnp.bfloat16)

    def halos(at):
        it, h = steps[at]
        flows = 3 if at + 1 == len(steps) else 4
        landed = tables[it][h].at[pl.ds(nblocks, flows * slots)]
        bytes_of(landed, send_sem.at[0], recv_sem.at[at]).wait_recv()

    gather_late()
    masses, g1 = [], None
    for at, (it, h) in enumerate(steps):
        if at + 1 < len(steps):
            relay_copy(*steps[at + 1]).wait_recv()
            forward_copy(*steps[at + 1]).start()
        final = h + 1 == halves
        if it == 1 and final:
            g1 = mass_total(0)
            masses = [blend_second(other, half_of(g1, other)) for other in range(h)]
        halos(at)
        if it == 0:
            masses.append(propagate(0, h))
        elif it == 1:
            propagate(1, h)
        elif not final:
            propagate(2, h, half_of(g1, h))
        else:
            g2 = mass_total(1)
            masses = list(propagate(2, h, half_of(g1, h), g2))
            bytes_of(late, send_sem.at[0], recv_sem.at[at + 1]).wait_recv()
            masses.append(propagate_late(h, half_of(g1, h), half_of(g2, h)))
        if it == 0 and final:
            mass_first(0, masses)
        if it == 1 and final:
            mass_first(1, masses + [blend_second(h, half_of(g1, h))])
    mass_first(2, masses)
    bytes_of(tiles.at[pl.ds(0, (5 * len(steps) - 1) * slots)], send_sem.at[0], recv_sem.at[0]).wait_send()
    bytes_of(got, mass_send.at[0], mass_recv.at[0]).wait_send()
    scale_ref[...] = mass_total(2)


def local(vp_count, rep_count, features, tile_values, tile_cols, halo_rows):
    tile_size = tile_values.shape[1]
    rows, classes = features.shape
    nblocks = rows // tile_size
    slots = halo_rows.shape[2]
    halves = classes // LANES
    shards = vp_count * rep_count
    block = (tile_size, LANES)
    bf16, f32 = jnp.bfloat16, jnp.float32
    each = ITERS * halves
    scratch = [pltpu.VMEM(tile_values.shape, bf16)]
    scratch += [pltpu.VMEM((nblocks + 4 * slots,) + block, bf16)] * each
    scratch += [pltpu.VMEM((nblocks,) + block, bf16)] * (2 * halves)
    scratch += [pltpu.VMEM((4 * slots,) + block, bf16)] * each
    scratch += [pltpu.VMEM((nblocks,) + block, f32)] * (2 * halves)
    scratch += [pltpu.VMEM((ITERS, 1, classes), f32), pltpu.VMEM((ITERS, shards - 1, 1, classes), f32)]
    scratch += [pltpu.VMEM((slots,) + block, bf16)] * each
    scratch += [pltpu.VMEM((nblocks, tile_size, slots * tile_size), bf16)]
    scratch += [pltpu.SMEM((nblocks,), jnp.int32), pltpu.SMEM((nblocks + 4 * slots,), jnp.int32)]
    scratch += [pltpu.SMEM(tile_cols.shape, jnp.int32), pltpu.SMEM(halo_rows.shape, jnp.int32)]
    dma = lambda *shape: pltpu.SemaphoreType.DMA(shape)
    scratch += [dma(2), dma(1), dma(halves), dma(halves), dma(1), dma(each + 1)]
    scratch += [dma(1), dma(ITERS), dma(each - 1)]
    operands = (tile_cols, halo_rows, features.reshape(nblocks, tile_size, classes), tile_values)
    finals, scale = pl.pallas_call(
        functools.partial(kernel, vp_count, rep_count, rows * shards, slots, halves),
        out_shape=(
            pltpu.VMEM((nblocks, tile_size, classes), f32),
            pltpu.VMEM((1, classes), f32),
        ),
        in_specs=[pl.BlockSpec(memory_space=pltpu.HBM)] * 4,
        out_specs=(pl.BlockSpec(memory_space=pltpu.VMEM),) * 2,
        scratch_shapes=scratch,
        compiler_params=pltpu.CompilerParams(
            collective_id=0, has_side_effects=True, vmem_limit_bytes=VMEM_LIMIT
        ),
    )(*[pltpu.with_memory_space_constraint(x, pltpu.HBM) for x in operands])
    return (finals * scale[None]).astype(bf16).reshape(rows, classes)


def solution(mesh):
    return jax.shard_map(
        functools.partial(local, mesh.shape["vp"], mesh.shape["rep"]),
        mesh=mesh,
        in_specs=(
            P(("vp", "rep"), None),
            P(("vp", "rep"), None, None),
            P(("vp", "rep")),
            P(("vp", "rep"), None, None),
        ),
        out_specs=P(("vp", "rep"), None),
        check_vma=False,
    )
```
